32 devices in a mesh: rep: 2 (over x), tp: 8 (over z, y), sub: 2 (over core).
Axes of the slice: x: 2, y: 2, z: 4, core: 2. Of those that a mesh axis runs over, the one named last changes fastest.
Arguments:
- attention: bfloat16 [1024, 8192], P('rep', ('tp', 'sub')), parts along dimension 0, may hold values from -6 to 6
- out_weight: bfloat16 [8192, 8192], P(('tp', 'sub')), may hold values from -0.09375 to 0.09375
- residual: bfloat16 [1024, 8192], P('rep', ('tp', 'sub')), parts along dimension 0, may hold values from -6 to 6
- norm_gain: bfloat16 [8192], P(('tp', 'sub')), may hold values from 0.25 to 1.75
Outputs:
- quantized: bfloat16 [1024, 8192], P('rep'), parts along dimension 0
- scales: bfloat16 [1024, 64], P('rep'), parts along dimension 0
- new_residual: bfloat16 [1024, 8192], P('rep', ('tp', 'sub')), parts along dimension 0
The draws below stay inside these ranges and needn't reach their ends.
There are 2 independent parts, one for each index of `rep`. The reference program is written for one: setup_inputs(seed, part) draws one part's arguments, and reference() takes and returns one part's arrays. A program takes and returns all parts, laid end to end along the dimension named above; an argument that names none is the same for every part. Nothing has to cross between parts.
All inputs are finite; a program needn't handle non-finite values.
Results may differ from the reference program's by a relative error of at most 0.0048.
Values may be sent and summed in bfloat16 or wider, within the bound.
No kernel may reach another device: no remote copies, remote signals or barrier semaphores. Data moves between devices by JAX's collectives and lax.ppermute only.
A program may use at most 128 MiB of HBM per device.

```python
import jax
import jax.numpy as jnp
from jax import lax

D = 8192
BLOCK = 128
ROWS = 512


def with_spikes(drawn, own_key, source, target, shards_of, factor):
    owner, partner = [(jnp.arange(drawn.shape[position]) // (drawn.shape[position] // shards_of)).reshape([-1 if axis == position else 1 for axis in range(drawn.ndim)]) for position in (source, target)]
    chosen = jax.random.permutation(own_key, shards_of)[partner]
    strong = (owner == chosen) | (owner == (partner + shards_of // 2) % shards_of)
    return jnp.where(strong, factor * drawn, drawn)


def block_scale(stream_key, shape, split, low, top_value):
    def one(dim, parts):
        steps = jax.random.uniform(jax.random.fold_in(jax.random.fold_in(stream_key, 6), dim), (parts,), jnp.float32, low / len(split), top_value / len(split))
        return jnp.repeat(jnp.exp(steps), shape[dim] // parts).reshape((-1,) + (1,) * (len(shape) - dim - 1))

    loudness = one(*split[0])
    for cut in split[1:]:
        loudness = loudness * one(*cut)
    return loudness


def gaussian(own_key, shape, width, most, pieces=(), dtype=jnp.bfloat16):
    array = width * jax.random.normal(own_key, shape, jnp.float32)
    if pieces:
        array = array * block_scale(own_key, shape, pieces, -0.22, 0.18)
    return jnp.clip(array, -most, most).astype(dtype)


def heavy_noise(own_key, shape, scale, limit, split, heavy, kind=jnp.bfloat16):
    entries = scale * jax.random.normal(own_key, shape, jnp.float32)
    if split:
        entries = entries * block_scale(own_key, shape, split, -0.22, 0.18)
    return jnp.clip(with_spikes(entries, jax.random.fold_in(own_key, 3), *heavy), -limit, limit).astype(kind)


def setup_inputs(seed: int = 0, part: int = 0) -> dict:
    key_of = jax.random.split(jax.random.key(seed), 5)
    own_keys = jax.random.split(jax.random.fold_in(key_of[4], part), 5)
    return {
        "attention": gaussian(own_keys[0], (ROWS, D), 1.0, 6.0, ((1, 16),)),
        "out_weight": heavy_noise(key_of[1], (D, D), D ** -0.5, 0.09375, ((0, 16),), (0, 1, 16, 2.0)),
        "residual": gaussian(own_keys[2], (ROWS, D), 1.0, 6.0, ((1, 16),)),
        "norm_gain": jnp.clip(1.0 + 0.15 * jax.random.normal(key_of[3], (D,), jnp.float32), 0.25, 1.75).astype(jnp.bfloat16),
    }


epsilon = 0.1
floor_scale = 0.5

def reference(attention, out_weight, residual, norm_gain):
    projected = jnp.dot(attention, out_weight, preferred_element_type=jnp.float32)
    hidden = residual.astype(jnp.float32) + projected
    new_residual = hidden.astype(jnp.bfloat16)
    mean_square = lax.optimization_barrier(jnp.mean(hidden * hidden, axis=1, keepdims=True))
    normed = hidden * lax.rsqrt(mean_square + epsilon) * norm_gain.astype(jnp.float32)
    blocks = normed.reshape(hidden.shape[0], hidden.shape[1] // BLOCK, BLOCK)
    largest = lax.optimization_barrier(jnp.max(jnp.abs(blocks), axis=2))
    scales = jnp.maximum(largest, floor_scale).astype(jnp.bfloat16)
    quantized = (blocks / scales.astype(jnp.float32)[:, :, None]).reshape(hidden.shape).astype(jnp.bfloat16)
    return (quantized, scales, new_residual)
```

```python
import functools

import jax
import jax.numpy as jnp
from jax import lax
from jax.experimental import pallas as pl
from jax.experimental.pallas import tpu as pltpu
from jax.sharding import PartitionSpec as P

BLOCK = 128
LANES = 128
TAIL = 8
SHORT_RING = 8

epsilon = 0.1
floor_scale = 0.5


def cost(flops, moved):
    return pl.CostEstimate(flops=int(flops), bytes_accessed=int(moved), transcendentals=0)


def ring_order(mesh):
    natural = list(range(mesh.shape["tp"]))
    snake = natural[0::2] + natural[1::2][::-1]
    place = [getattr(d, "coords", None) for d in mesh.devices[0, :, 0]]
    if None in place:
        return natural

    def length(order):
        pairs = zip(order, order[1:] + order[:1])
        return sum(sum(abs(i - j) for i, j in zip(place[a], place[b])) for a, b in pairs)

    return min((natural, snake), key=length)


def pick_kernel(width, spot, weight, out, sem):
    copies = []
    for k in range(out.shape[0]):
        column = pl.multiple_of(spot[k] * width, width)
        copies.append(pltpu.make_async_copy(weight.at[:, pl.ds(column, width)], out.at[k], sem.at[k]))
    for copy in copies:
        copy.start()
    for copy in copies:
        copy.wait()


def partial_kernel(spot, own, far, weight_own, weight_far, top, bottom):
    half = top.shape[1]
    for k, out in enumerate((top, bottom)):
        part = pl.ds(k * half, half)
        total = jnp.dot(own[part, :], weight_own[...], preferred_element_type=jnp.float32)
        total = total + jnp.dot(far[part, :], weight_far[0], preferred_element_type=jnp.float32)
        out[0] = total.astype(out.dtype)


def hidden_kernel(own, residual, first, second, hidden, rounded, squares):
    rows, width = hidden.shape
    for row in range(0, rows, LANES):
        part = pl.ds(row, LANES)
        value = own[0, part, :] + residual[part, :].astype(jnp.float32)
        value = value + first[part, :].astype(jnp.float32) + second[part, :].astype(jnp.float32)
        hidden[part, :] = value
        rounded[part, :] = value.astype(jnp.bfloat16)
        square = value * value
        total = square[:, :LANES]
        for column in range(LANES, width, LANES):
            total = total + square[:, column : column + LANES]
        squares[0:1, part] = jnp.sum(total.T, axis=0, keepdims=True)


def quantize_kernel(width_all, squares, hidden, gain, out):
    rows, width = hidden.shape
    per = width // BLOCK
    lane = lax.broadcasted_iota(jnp.int32, (LANES, LANES), 1)
    for chunk in range(rows // LANES):
        part = pl.ds(chunk * LANES, LANES)
        inverse = lax.rsqrt(squares[0:1, part] / width_all + epsilon)
        inverse = jnp.broadcast_to(inverse, (LANES, LANES)).T
        gathered = jnp.zeros((LANES, LANES), jnp.float32)
        for b in range(per):
            columns = pl.ds(b * BLOCK, BLOCK)
            normed = hidden[part, columns] * inverse * gain[0:1, columns].astype(jnp.float32)
            largest = jnp.max(jnp.abs(normed), axis=1, keepdims=True)
            scale = jnp.maximum(largest, floor_scale).astype(jnp.bfloat16).astype(jnp.float32)
            out[part, columns] = (normed / scale).astype(jnp.bfloat16)
            gathered = jnp.where(lane == b, scale, gathered)
        line, column = divmod(chunk, width // LANES)
        turned = gathered.T.astype(jnp.bfloat16)
        out[pl.ds(rows + line * per, per), pl.ds(column * LANES, LANES)] = turned[:per]


def place_kernel(starts, fresh, spot, *refs):
    blocks = refs[: len(starts)]
    full, tails, sem = refs[-3:]
    copies = []
    for k, (start, block) in enumerate(zip(starts, blocks)):
        rows, width = block.shape[0] - TAIL, block.shape[1]
        column = pl.multiple_of(spot[k] * width, width)
        line = pl.multiple_of(spot[k] * TAIL, TAIL)
        copies.append(
            pltpu.make_async_copy(
                block.at[pl.ds(0, rows)],
                full.at[pl.ds(start * rows, rows), pl.ds(column, width)],
                sem.at[0, k],
            )
        )
        copies.append(
            pltpu.make_async_copy(block.at[pl.ds(rows, TAIL)], tails.at[start, pl.ds(line, TAIL)], sem.at[1, k])
        )
    for copy in copies:
        copy.start()
    for copy in copies:
        copy.wait()


def make_per_device(mesh):
    order = ring_order(mesh)
    n, m = mesh.shape["tp"], mesh.shape["sub"]
    link_type = jnp.bfloat16 if n <= SHORT_RING else jnp.float32
    where = [order.index(t) for t in range(n)]
    far = n // 2

    def forward(x, hops):
        return lax.ppermute(x, "tp", [(order[i], order[(i + hops) % n]) for i in range(n)])

    def across(x):
        return lax.ppermute(x, "sub", [(i, (i + 1) % m) for i in range(m)])

    def everywhere(x):
        x = x + across(x)
        bit = 1
        while bit < n:
            x = x + lax.ppermute(x, "tp", [(t, t ^ bit) for t in range(n)])
            bit *= 2
        return x

    def per_device(attention, out_weight, residual, norm_gain):
        rows, width = residual.shape
        depth, width_all = out_weight.shape
        half = rows // 2
        per = width // BLOCK
        tp, core = lax.axis_index("tp"), lax.axis_index("sub")
        other = (core + 1) % m
        position = jnp.array(where, jnp.int32)[tp]
        owners = jnp.array(order, jnp.int32)

        def spots(hops, which):
            return owners[(position + jnp.array(hops, jnp.int32)) % n] * m + which

        def pick(hops):
            count = len(hops)
            return pl.pallas_call(
                functools.partial(pick_kernel, width),
                in_specs=[pl.BlockSpec(memory_space=pltpu.SMEM), pl.BlockSpec(memory_space=pl.ANY)],
                out_specs=pl.BlockSpec(memory_space=pltpu.VMEM),
                out_shape=jax.ShapeDtypeStruct((count, depth, width), jnp.bfloat16),
                scratch_shapes=[pltpu.SemaphoreType.DMA((count,))],
                compiler_params=pltpu.CompilerParams(vmem_limit_bytes=8 << 20),
                cost_estimate=cost(count * 1e8, count * depth * width * 4),
            )(spots(hops, other), out_weight)

        attention_far = across(attention)

        def partials(hops, out_type):
            count = len(hops)
            weight_far = across(pick(hops))
            return pl.pallas_call(
                partial_kernel,
                grid_spec=pltpu.PrefetchScalarGridSpec(
                    num_scalar_prefetch=1,
                    grid=(count,),
                    in_specs=[
                        pl.BlockSpec((rows, depth), lambda i, spot: (0, 0)),
                        pl.BlockSpec((rows, depth), lambda i, spot: (0, 0)),
                        pl.BlockSpec((depth, width), lambda i, spot: (0, spot[i])),
                        pl.BlockSpec((1, depth, width), lambda i, spot: (i, 0, 0)),
                    ],
                    out_specs=[pl.BlockSpec((1, half, width), lambda i, spot: (i, 0, 0))] * 2,
                ),
                out_shape=[jax.ShapeDtypeStruct((count, half, width), out_type)] * 2,
                compiler_params=pltpu.CompilerParams(vmem_limit_bytes=16 << 20),
                cost_estimate=cost(4 * count * rows * depth * width, 4 * count * depth * width),
            )(spots(hops, core), attention, attention_far, out_weight, weight_far)

        groups = [[far], [far - 1, 1 - far], [s * k for k in range(far - 2, 0, -1) for s in (1, -1)] + [0]]
        groups = [[k for k in group if -far < k <= far] for group in groups]
        terms = {}
        for g, group in enumerate(groups):
            halves = partials(group, jnp.float32 if g else link_type)
            for i, k in enumerate(group):
                terms[k % n] = [h[i] for h in halves]
            own = halves

        arrived = {}
        for k in range(far, 0, -1):
            for part, sign in ((0, 1), (1, -1)):
                for direction in (sign, -sign):
                    if k == far and direction != sign:
                        continue
                    term = terms[direction * k % n][part]
                    if (part, direction) in arrived:
                        term = term + arrived[part, direction].astype(jnp.float32)
                    arrived[part, direction] = forward(term.astype(link_type), direction)

        hiddens, residuals, squares = [], [], []
        for part in range(2):
            hidden, rounded, square = pl.pallas_call(
                hidden_kernel,
                grid=(1,),
                in_specs=[
                    pl.BlockSpec((1, half, width), lambda i: (len(groups[-1]) - 1, 0, 0)),
                    pl.BlockSpec((half, width), lambda i, part=part: (part, 0)),
                    pl.BlockSpec((half, width), lambda i: (0, 0)),
                    pl.BlockSpec((half, width), lambda i: (0, 0)),
                ],
                out_specs=[
                    pl.BlockSpec((half, width), lambda i: (0, 0)),
                    pl.BlockSpec((half, width), lambda i: (0, 0)),
                    pl.BlockSpec((1, half), lambda i: (0, 0)),
                ],
                out_shape=[
                    jax.ShapeDtypeStruct((half, width), jnp.float32),
                    jax.ShapeDtypeStruct((half, width), jnp.bfloat16),
                    jax.ShapeDtypeStruct((1, half), jnp.float32),
                ],
                compiler_params=pltpu.CompilerParams(vmem_limit_bytes=16 << 20),
                cost_estimate=cost(1e8, 8 * half * width),
            )(own[part], residual, arrived[part, 1], arrived[part, -1])
            hiddens.append(hidden)
            residuals.append(rounded)
            squares.append(square)
        square = everywhere(jnp.concatenate(squares, axis=0))

        full = tails = None

        def place(pieces, full, tails):
            starts = [part for part, _, _ in pieces]
            blocks = [block for _, _, block in pieces]
            spot = jnp.concatenate([spots([hop], which) for _, (hop, which), _ in pieces])
            shapes = [
                jax.ShapeDtypeStruct((rows, width_all), jnp.bfloat16),
                jax.ShapeDtypeStruct((2, n * m * TAIL, width), jnp.bfloat16),
            ]
            more = [] if full is None else [full, tails]
            return pl.pallas_call(
                functools.partial(place_kernel, starts, not more),
                in_specs=[pl.BlockSpec(memory_space=pltpu.SMEM)]
                + [pl.BlockSpec(memory_space=pltpu.VMEM)] * len(blocks)
                + [pl.BlockSpec(memory_space=pl.ANY)] * len(more),
                out_specs=[pl.BlockSpec(memory_space=pl.ANY)] * 2,
                out_shape=shapes,
                scratch_shapes=[pltpu.SemaphoreType.DMA((2, len(blocks)))],
                input_output_aliases={1 + len(blocks): 0, 2 + len(blocks): 1} if more else {},
                compiler_params=pltpu.CompilerParams(vmem_limit_bytes=16 << 20),
                cost_estimate=cost(1e8, 4 * len(blocks) * half * width),
            )(spot, *blocks, *more)

        held = {}
        for part in range(2):
            held[part, 1] = held[part, -1] = pl.pallas_call(
                functools.partial(quantize_kernel, width_all),
                grid=(1,),
                in_specs=[
                    pl.BlockSpec((1, half), lambda i: (0, 0)),
                    pl.BlockSpec((half, width), lambda i: (0, 0)),
                    pl.BlockSpec((1, width), lambda i: (0, 0)),
                ],
                out_specs=pl.BlockSpec((half + TAIL, width), lambda i: (0, 0)),
                out_shape=jax.ShapeDtypeStruct((half + TAIL, width), jnp.bfloat16),
                compiler_params=pltpu.CompilerParams(vmem_limit_bytes=16 << 20),
                cost_estimate=cost(1e8, 8 * half * width),
            )(square[part : part + 1], hiddens[part], norm_gain[None])
        pieces = []
        for part in range(2):
            block = held[part, 1]
            pieces += [(part, (0, core), block), (part, (0, other), across(block))]
        waiting = pieces
        for k in range(1, far + 1):
            pieces = []
            for part, sign in ((0, 1), (1, -1)):
                for direction in (sign, -sign):
                    if k == far and direction != sign:
                        continue
                    block = held[part, direction] = forward(held[part, direction], direction)
                    hop = -direction * k
                    pieces += [(part, (hop, core), block), (part, (hop, other), across(block))]
            full, tails = place(waiting, full, tails)
            waiting = pieces
        full, tails = place(waiting, full, tails)
        fold = max(1, half // width)
        scales = tails.reshape(2, n * m, TAIL, width)[:, :, : per * fold, : min(half, width)]
        scales = scales.reshape(2, n * m, fold, per, half // fold).transpose(1, 3, 0, 2, 4)
        return (full, scales.reshape(n * m * per, rows).T, jnp.concatenate(residuals, axis=0))

    return per_device


def solution(mesh):
    in_specs = (
        P("rep", ("tp", "sub")),
        P(("tp", "sub"), None),
        P("rep", ("tp", "sub")),
        P(("tp", "sub")),
    )
    out_specs = (P("rep", None), P("rep", None), P("rep", ("tp", "sub")))
    return jax.shard_map(
        make_per_device(mesh), mesh=mesh, in_specs=in_specs, out_specs=out_specs, check_vma=False
    )
```
